32 devices in a mesh: rep: 16 (over z, y, core), tp: 2 (over x).
Axes of the slice: x: 2, y: 2, z: 4, core: 2. Of those that a mesh axis runs over, the one named last changes fastest.
Arguments:
- activations: bfloat16 [8192, 6144], P('rep', 'tp'), may hold values from -6 to 6
- norm_gain: float32 [6144], replicated, may hold values from 0.5 to 1.5
- query_gain: float32 [128], replicated, may hold values from 0.5 to 18
- key_gain: float32 [128], replicated, may hold values from 0.5 to 18
- project_in: bfloat16 [6144, 24, 384], P('rep', 'tp'), may hold values from -1 to 1
- project_out: bfloat16 [6144, 3072], P('rep', 'tp'), may hold values from -1 to 1
Outputs:
- attended: bfloat16 [8192, 6144], P('rep', 'tp')
- weight_norms: float32 [2], replicated
The draws below stay inside these ranges and needn't reach their ends.
All inputs are finite; a program needn't handle non-finite values.
Results may differ from the reference program's by a relative error of at most 0.018.
The reference program's roundings to bfloat16 on the way count: a program that leaves them out, or rounds other values in their place, can miss the bound.
Values may be sent and summed in bfloat16 or wider, within the bound.
A program may use at most 192 MiB of HBM per device.

```python
import math
import jax
import jax.numpy as jnp
from jax import lax

D = 6144
HEADS = 24
HEAD_DIM = 128
PATCHES = 256
IMG_REP = 2
TOKENS = 8192
N_REP = 16
N_TP = 2


def gain_common(key, salt):
    inner = jax.random.fold_in(key, salt)
    base = jax.random.uniform(inner, (HEAD_DIM,), jnp.float32, 0.5, 1.5)
    return base


def draw_query_gain(key, part):
    return gain_common(key, 11)


def draw_key_gain(key, part):
    return gain_common(key, 23)


def rising_rows(key, salt, columns, fan_in):
    inner = jax.random.fold_in(key, salt)
    entries = jax.random.truncated_normal(inner, -4.0, 4.0, (D, columns), jnp.float32)
    factor = 5.0
    place = jnp.arange(D).astype(jnp.float32) / (D - 1)
    scales = 1.0 + (factor - 1.0) * place
    scales = scales / jnp.sqrt(jnp.mean(scales * scales))
    return entries * scales[:, None] * fan_in ** (-0.5)


def draw_project_in(key, part):
    values = rising_rows(key, 31, HEADS * 3 * HEAD_DIM, D)
    return values.reshape(D, HEADS, 3 * HEAD_DIM).astype(jnp.bfloat16)


def draw_project_out(key, part):
    return rising_rows(key, 47, HEADS * HEAD_DIM, HEADS * HEAD_DIM).astype(jnp.bfloat16)


def steps_of(rng, dims, pieces, low, high):
    def one(axis_at, parts):
        steps = jax.random.uniform(jax.random.fold_in(jax.random.fold_in(rng, 6), axis_at), (parts,), jnp.float32, low / len(pieces), high / len(pieces))
        return jnp.repeat(jnp.exp(steps), dims[axis_at] // parts).reshape((-1,) + (1,) * (len(dims) - axis_at - 1))

    loudness = one(*pieces[0])
    for cut in pieces[1:]:
        loudness = loudness * one(*cut)
    return loudness


def gaussian(key, dims, deviation, most, pieces=(), dtype=jnp.bfloat16):
    result = deviation * jax.random.normal(key, dims, jnp.float32)
    if pieces:
        result = result * steps_of(key, dims, pieces, -0.22, 0.18)
    return jnp.clip(result, -most, most).astype(dtype)


def setup_inputs(seed: int = 0) -> dict:
    arg_keys = jax.random.split(jax.random.key(seed), 7)
    return {
        "activations": gaussian(arg_keys[0], (TOKENS, D), 1.0, 6.0, ((0, 16), (1, 2))),
        "norm_gain": jnp.clip(1.0 + 0.1 * jax.random.normal(arg_keys[1], (D,), jnp.float32), 0.5, 1.5),
        "query_gain": draw_query_gain(jax.random.fold_in(arg_keys[6], 71), 0),
        "key_gain": draw_key_gain(jax.random.fold_in(arg_keys[6], 71), 0),
        "project_in": draw_project_in(jax.random.fold_in(arg_keys[6], 71), 0),
        "project_out": draw_project_out(jax.random.fold_in(arg_keys[6], 71), 0),
    }


def layer_norm(values, gain):
    average = lax.optimization_barrier(jnp.mean(values, -1, keepdims=True))
    centred = values - average
    variance = lax.optimization_barrier(jnp.mean(centred * centred, -1, keepdims=True))
    return centred * lax.rsqrt(variance + 1e-06) * gain

def reference(activations, norm_gain, query_gain, key_gain, project_in, project_out):
    normed = layer_norm(activations.astype(jnp.float32), norm_gain).astype(jnp.bfloat16)
    projection = project_in.reshape(D, HEADS * 3 * HEAD_DIM)

    def one_image(patches_in):
        projected = jnp.dot(patches_in, projection, preferred_element_type=jnp.float32)
        projected = projected.reshape(PATCHES, HEADS, 3 * HEAD_DIM)
        queries = layer_norm(projected[..., :HEAD_DIM], query_gain).astype(jnp.bfloat16)
        keys_normed = layer_norm(projected[..., HEAD_DIM:2 * HEAD_DIM], key_gain).astype(jnp.bfloat16)
        values = projected[..., 2 * HEAD_DIM:].astype(jnp.bfloat16)
        scores = jnp.einsum('phd,qhd->hpq', queries.astype(jnp.float32), keys_normed.astype(jnp.float32)) / math.sqrt(HEAD_DIM)
        probabilities = jax.nn.softmax(scores, axis=-1).astype(jnp.bfloat16)
        mixed = jnp.einsum('hpq,qhd->phd', probabilities.astype(jnp.float32), values.astype(jnp.float32))
        return mixed.astype(jnp.bfloat16).reshape(PATCHES, HEADS * HEAD_DIM)
    mixed = lax.map(one_image, normed.reshape(IMG_REP * N_REP, PATCHES, D))
    mixed = mixed.reshape(IMG_REP * N_REP * PATCHES, HEADS * HEAD_DIM)
    columns_each = HEADS * HEAD_DIM // N_TP
    total = jnp.zeros((mixed.shape[0], D), jnp.float32)
    for group_index in range(N_TP):
        lower = group_index * columns_each
        partial_value = lax.dot_general(mixed[:, lower:lower + columns_each], project_out[:, lower:lower + columns_each], (((1,), (1,)), ((), ())), preferred_element_type=jnp.float32)
        partial_value = lax.optimization_barrier(partial_value.astype(jnp.bfloat16))
        total = total + partial_value.astype(jnp.float32)
    attended = total.astype(jnp.bfloat16)
    weight_norms = jnp.stack([jnp.sqrt(jnp.sum(jnp.square(project_in.astype(jnp.float32))) / (3 * HEADS * HEAD_DIM)), jnp.sqrt(jnp.sum(jnp.square(project_out.astype(jnp.float32))) / D)])
    return (attended, weight_norms)
```

```python
import functools
import math

import jax
import jax.numpy as jnp
from jax import lax
from jax.sharding import PartitionSpec as P

D = 6144
HEADS = 24
HEAD_DIM = 128
PATCHES = 256


def layer_norm(values, gain):
    average = jnp.mean(values, -1, keepdims=True)
    centred = values - average
    variance = jnp.mean(centred * centred, -1, keepdims=True)
    return centred * lax.rsqrt(variance + 1e-06) * gain


def heads_mixed(projected, query_gain, key_gain, head_dim):
    tok_rows, width = projected.shape
    heads = width // (3 * head_dim)
    projected = projected.reshape(tok_rows // PATCHES, PATCHES, heads, 3 * head_dim)
    queries = layer_norm(projected[..., :head_dim], query_gain).astype(jnp.bfloat16)
    keys_normed = layer_norm(projected[..., head_dim : 2 * head_dim], key_gain).astype(jnp.bfloat16)
    values = projected[..., 2 * head_dim :].astype(jnp.bfloat16)
    scores = jnp.einsum(
        "iphd,iqhd->ihpq", queries, keys_normed, preferred_element_type=jnp.float32
    ) / math.sqrt(head_dim)
    probabilities = jax.nn.softmax(scores, axis=-1).astype(jnp.bfloat16)
    mixed = jnp.einsum("ihpq,iqhd->iphd", probabilities, values, preferred_element_type=jnp.float32)
    return mixed.astype(jnp.bfloat16).reshape(tok_rows, heads * head_dim)


def chunk_count(size, wanted):
    while size % wanted:
        wanted -= 1
    return wanted


def shards(n_rep, n_tp, activations, norm_gain, query_gain, key_gain, project_in, project_out):
    me = lax.axis_index("tp")
    swap = [(0, 1), (1, 0)]
    local_rows, local_heads, head_width = project_in.shape
    head_dim = head_width // 3

    n_in = chunk_count(local_heads, 3)
    step = local_heads // n_in
    pieces = []
    for j in range(n_in):
        part = project_in[:, j * step : (j + 1) * step].reshape(local_rows, step * head_width)
        pieces.append(lax.all_gather(part, "rep", axis=0, tiled=True))
    out_rows, out_depth = project_out.shape
    n_out = chunk_count(out_rows // 128, 3) if out_rows % 128 == 0 else 1
    span = out_rows // n_out
    out_pieces = []
    for j in range(n_out):
        part = project_out[j * span : (j + 1) * span]
        out_pieces.append(lax.all_gather(part, "rep", axis=0, tiled=True))

    local_in = jnp.sum(jnp.square(project_in.astype(jnp.float32)))
    local_out = jnp.sum(jnp.square(project_out.astype(jnp.float32)))
    totals = lax.psum(jnp.stack([local_in, local_out]), ("rep", "tp"))
    if n_tp == 2:
        other = lax.ppermute(activations, "tp", swap)
        other, totals = lax.optimization_barrier((other, totals))
        first = jnp.where(me == 0, activations, other)
        second = jnp.where(me == 0, other, activations)
        gathered_rows = jnp.concatenate([first, second], axis=1)
    else:
        gathered_rows = lax.all_gather(activations, "tp", axis=1, tiled=True)
    normed = layer_norm(gathered_rows.astype(jnp.float32), norm_gain).astype(jnp.bfloat16)

    mixed = []
    for piece in pieces:
        projected = jnp.dot(normed, piece, preferred_element_type=jnp.float32)
        mixed.append(heads_mixed(projected, query_gain, key_gain, head_dim))
    mixed = jnp.concatenate(mixed, axis=1)

    def product(rows):
        total = lax.dot_general(
            mixed, rows, (((1,), (1,)), ((), ())), preferred_element_type=jnp.float32
        )
        return total.astype(jnp.bfloat16)

    sums = []
    for piece in out_pieces:
        if n_tp == 2:
            half = piece.shape[0] // 2
            sent = product(lax.dynamic_slice_in_dim(piece, (1 - me) * half, half, 0))
            arrived = lax.ppermute(sent, "tp", swap)
            kept = product(lax.dynamic_slice_in_dim(piece, me * half, half, 0))
            total = kept.astype(jnp.float32) + arrived.astype(jnp.float32)
            sums.append(total.astype(jnp.bfloat16))
        else:
            sums.append(lax.psum_scatter(product(piece), "tp", scatter_dimension=1, tiled=True))
    owners = n_rep // n_tp
    blocks = [sums[j][:, r * span : (r + 1) * span] for r in range(owners) for j in range(n_out)]
    attended = jnp.concatenate(blocks, axis=1)
    fans = jnp.array([3 * HEADS * HEAD_DIM, D], jnp.float32)
    return (attended, jnp.sqrt(totals / fans))


def solution(mesh):
    in_specs = (P("rep", "tp"), P(), P(), P(), P("rep", "tp", None), P("rep", "tp"))
    out_specs = (P("rep", "tp"), P())
    body = functools.partial(shards, mesh.shape["rep"], mesh.shape["tp"])
    return jax.shard_map(body, mesh=mesh, in_specs=in_specs, out_specs=out_specs, check_vma=False)
```

```python
import math

import jax
import jax.numpy as jnp
from jax import lax
from jax.sharding import PartitionSpec as P

D = 6144
HEADS = 24
HEAD_DIM = 128
PATCHES = 256


def layer_norm(values, gain):
    average = jnp.mean(values, -1, keepdims=True)
    centred = values - average
    variance = jnp.mean(centred * centred, -1, keepdims=True)
    return centred * lax.rsqrt(variance + 1e-06) * gain


def heads_mixed(projected, query_gain, key_gain, head_dim):
    tok_rows, width = projected.shape
    heads = width // (3 * head_dim)
    projected = projected.reshape(tok_rows // PATCHES, PATCHES, heads, 3 * head_dim)
    queries = layer_norm(projected[..., :head_dim], query_gain).astype(jnp.bfloat16)
    keys_normed = layer_norm(projected[..., head_dim : 2 * head_dim], key_gain).astype(jnp.bfloat16)
    values = projected[..., 2 * head_dim :].astype(jnp.bfloat16)
    scores = jnp.einsum(
        "iphd,iqhd->ihpq", queries, keys_normed, preferred_element_type=jnp.float32
    ) / math.sqrt(head_dim)
    probabilities = jax.nn.softmax(scores, axis=-1).astype(jnp.bfloat16)
    mixed = jnp.einsum("ihpq,iqhd->iphd", probabilities, values, preferred_element_type=jnp.float32)
    return mixed.astype(jnp.bfloat16).reshape(tok_rows, heads * head_dim)


def chunk_count(size, wanted):
    while size % wanted:
        wanted -= 1
    return wanted


def shards(n_rep, n_tp, activations, norm_gain, query_gain, key_gain, project_in, project_out):
    me = lax.axis_index("tp")
    swap = [(0, 1), (1, 0)]
    local_rows, local_heads, head_width = project_in.shape
    head_dim = head_width // 3

    n_in = chunk_count(local_heads, 3)
    step = local_heads // n_in
    pieces = []
    for j in range(n_in):
        part = project_in[:, j * step : (j + 1) * step].reshape(local_rows, step * head_width)
        pieces.append(lax.all_gather(part, "rep", axis=0, tiled=True))
    out_rows, out_depth = project_out.shape
    n_out = chunk_count(out_rows // 128, 3) if out_rows % 128 == 0 else 1
    span = out_rows // n_out
    out_pieces = []
    for j in range(n_out):
        part = project_out[j * span : (j + 1) * span]
        out_pieces.append(lax.all_gather(part, "rep", axis=0, tiled=True))

    local_in = jnp.sum(jnp.square(project_in.astype(jnp.float32)))
    local_out = jnp.sum(jnp.square(project_out.astype(jnp.float32)))
    totals = lax.psum(jnp.stack([local_in, local_out]), ("rep", "tp"))
    if n_tp == 2:
        other = lax.ppermute(activations, "tp", swap)
        other, totals = lax.optimization_barrier((other, totals))
        first = jnp.where(me == 0, activations, other)
        second = jnp.where(me == 0, other, activations)
        gathered_rows = jnp.concatenate([first, second], axis=1)
    else:
        gathered_rows = lax.all_gather(activations, "tp", axis=1, tiled=True)
    normed = layer_norm(gathered_rows.astype(jnp.float32), norm_gain).astype(jnp.bfloat16)

    mixed = []
    for piece in pieces:
        projected = jnp.dot(normed, piece, preferred_element_type=jnp.float32)
        mixed.append(heads_mixed(projected, query_gain, key_gain, head_dim))
    mixed = jnp.concatenate(mixed, axis=1)

    def product(rows):
        total = lax.dot_general(
            mixed, rows, (((1,), (1,)), ((), ())), preferred_element_type=jnp.float32
        )
        return total.astype(jnp.bfloat16)

    sums = []
    for piece in out_pieces:
        if n_tp == 2:
            half = piece.shape[0] // 2
            sent = product(lax.dynamic_slice_in_dim(piece, (1 - me) * half, half, 0))
            arrived = lax.ppermute(sent, "tp", swap)
            kept = product(lax.dynamic_slice_in_dim(piece, me * half, half, 0))
            total = kept.astype(jnp.float32) + arrived.astype(jnp.float32)
            sums.append(total.astype(jnp.bfloat16))
        else:
            sums.append(lax.psum_scatter(product(piece), "tp", scatter_dimension=1, tiled=True))
    owners = n_rep // n_tp
    blocks = [sums[j][:, r * span : (r + 1) * span] for r in range(owners) for j in range(n_out)]
    attended = jnp.concatenate(blocks, axis=1)
    fans = jnp.array([3 * HEADS * HEAD_DIM, D], jnp.float32)
    return (attended, jnp.sqrt(totals / fans))


def paired_shards(n_rep, activations, norm_gain, query_gain, key_gain, project_in, project_out):
    tp_me, rep_me = lax.axis_index("tp"), lax.axis_index("rep")
    core, y, z = rep_me % 2, (rep_me // 2) % 2, rep_me // 4
    n_z = n_rep // 4
    tp_swap = [(0, 1), (1, 0)]
    y_swap = [(i, i ^ 2) for i in range(n_rep)]
    core_swap = [(i, i ^ 1) for i in range(n_rep)]
    z_ring = [(i, (i + 4) % n_rep) for i in range(n_rep)]
    local_rows, local_heads, head_width = project_in.shape
    head_dim = head_width // 3
    some = local_heads // 2
    width = some * head_width

    def head_half(which):
        part = lax.dynamic_slice_in_dim(project_in, which * some, some, 1)
        return part.reshape(local_rows, width)

    chain_keep = [head_half(y)]
    chain_got = [lax.ppermute(head_half(1 - y), "rep", y_swap)]
    for k in range(n_z - 1):
        chain_keep.append(lax.ppermute(chain_keep[-1], "rep", z_ring))
        chain_got.append(lax.ppermute(chain_got[-1], "rep", z_ring))
    own_out, _ = lax.optimization_barrier((project_out, chain_keep[-1]))
    chain_out = [own_out]
    for k in range(n_z - 1):
        chain_out.append(lax.ppermute(chain_out[-1], "rep", z_ring))

    def rows_of(rows):
        other = lax.ppermute(rows, "tp", tp_swap)
        first = jnp.where(tp_me == 0, rows, other)
        second = jnp.where(tp_me == 0, other, rows)
        full = jnp.concatenate([first, second], axis=1)
        return layer_norm(full.astype(jnp.float32), norm_gain).astype(jnp.bfloat16)

    mine = rows_of(activations)
    theirs = rows_of(lax.ppermute(activations, "rep", y_swap))

    flips = [(0, 0), (1, 0), (0, 1), (1, 1)]

    def columns(normed, k):
        base = ((z - k) % n_z) * 4
        starts = [(base + (y ^ yb) * 2 + (core ^ cb)) * local_rows for yb, cb in flips]
        return jnp.concatenate(
            [lax.dynamic_slice_in_dim(normed, at, local_rows, 1) for at in starts], axis=1
        )

    sum_mine = sum_theirs = None
    for k in range(n_z):
        keep, got = chain_keep[k], chain_got[k]
        block = jnp.concatenate(
            [keep, got, lax.ppermute(keep, "rep", core_swap), lax.ppermute(got, "rep", core_swap)]
        )
        theirs_k = jnp.dot(columns(theirs, k), block, preferred_element_type=jnp.float32)
        mine_k = jnp.dot(columns(mine, k), block, preferred_element_type=jnp.float32)
        sum_theirs = theirs_k if sum_theirs is None else sum_theirs + theirs_k
        sum_mine = mine_k if sum_mine is None else sum_mine + mine_k
    mixed_theirs = heads_mixed(sum_theirs, query_gain, key_gain, head_dim)
    arrived = lax.ppermute(mixed_theirs, "rep", y_swap)
    mixed_mine = heads_mixed(sum_mine, query_gain, key_gain, head_dim)
    low = jnp.where(y == 0, mixed_mine, arrived)
    high = jnp.where(y == 0, arrived, mixed_mine)
    mixed = jnp.concatenate([low, high], axis=1)

    products = []
    for k in range(n_z):
        here = chain_out[k]
        there = lax.ppermute(here, "rep", y_swap)
        block = jnp.concatenate(
            [here, there, lax.ppermute(here, "rep", core_swap), lax.ppermute(there, "rep", core_swap)]
        )
        total = lax.dot_general(
            mixed, block, (((1,), (1,)), ((), ())), preferred_element_type=jnp.float32
        )
        products.append(total.astype(jnp.bfloat16))
    sums = []
    for k in range(n_z // 2):
        ours = ((z - k) % n_z) // (n_z // 2) == tp_me
        sent = jnp.where(ours, products[k + n_z // 2], products[k])
        kept = jnp.where(ours, products[k], products[k + n_z // 2])
        other = lax.ppermute(sent, "tp", tp_swap)
        sums.append((kept.astype(jnp.float32) + other.astype(jnp.float32)).astype(jnp.bfloat16))
    sums = jnp.concatenate(sums, axis=1)
    out_rows = project_out.shape[0]
    pieces = []
    for zl in range(n_z // 2):
        for yb in range(2):
            for cb in range(2):
                at = ((z - zl) % (n_z // 2)) * 4 + (core ^ cb) * 2 + (y ^ yb)
                pieces.append(lax.dynamic_slice_in_dim(sums, at * out_rows, out_rows, 1))
    attended = jnp.concatenate(pieces, axis=1)

    local_in = jnp.sum(jnp.square(project_in.astype(jnp.float32)))
    local_out = jnp.sum(jnp.square(project_out.astype(jnp.float32)))
    totals = jnp.stack([local_in, local_out])
    stride = 1
    while stride < n_rep:
        totals = totals + lax.ppermute(totals, "rep", [(i, i ^ stride) for i in range(n_rep)])
        stride *= 2
    totals = totals + lax.ppermute(totals, "tp", tp_swap)
    fans = jnp.array([3 * HEADS * HEAD_DIM, D], jnp.float32)
    return (attended, jnp.sqrt(totals / fans))


def solution(mesh):
    in_specs = (P("rep", "tp"), P(), P(), P(), P("rep", "tp", None), P("rep", "tp"))
    out_specs = (P("rep", "tp"), P())
    n_rep, n_tp = mesh.shape["rep"], mesh.shape["tp"]

    def body(*args):
        if n_tp == 2 and n_rep >= 8 and n_rep & (n_rep - 1) == 0 and args[4].shape[1] % 2 == 0:
            return paired_shards(n_rep, *args)
        return shards(n_rep, n_tp, *args)

    return jax.shard_map(body, mesh=mesh, in_specs=in_specs, out_specs=out_specs, check_vma=False)
```
